32 devices in a mesh: gx: 8 (over z, x), gy: 4 (over y, core).
Axes of the slice: x: 2, y: 2, z: 4, core: 2. Of those that a mesh axis runs over, the one named last changes fastest.
Arguments:
- orbitals: bfloat16 [20000, 200], P('gx'), may hold values from -6 to 6
- projector: bfloat16 [6016, 20000], P('gy', 'gx'), may hold values from -0.0390625 to 0.0390625
- integrals: bfloat16 [8, 6016, 6016], P('gx', 'gy'), may hold values from -1 to 1
Outputs:
- exchange_matrix: float32 [6016, 6016], P('gx', 'gy')
- exchange_orbitals: float32 [20000, 200], P('gx', 'gy')
- energy_mean: float32 [], replicated
- trace_mean: float32 [], replicated
The draws below stay inside these ranges and needn't reach their ends.
All inputs are finite; a program needn't handle non-finite values.
Results may differ from the reference program's by a relative error of at most 0.008.
Values may be sent and summed in bfloat16 or wider, within the bound.
A program may use at most 128 MiB of HBM per device.

```python
import jax
import jax.numpy as jnp
from jax import lax

NAO = 20000
NADM = 6016
NOCC = 200
NAUX = 8


def draw_integrals(key, part):
    keyed = jax.random.fold_in(key, 11)
    first = jax.random.fold_in(keyed, 0)
    shape = (NAUX, NADM, NADM)
    base = jax.random.normal(first, shape, jnp.float32)
    aux_scale = 0.5 + jnp.arange(NAUX, dtype=jnp.float32) / max(NAUX - 1, 1)
    row_scale = 0.5 + jnp.arange(NADM, dtype=jnp.float32) / max(NADM - 1, 1)
    sigma = (NADM * NOCC * NAUX) ** (-0.5)
    values = base * aux_scale[:, None, None] * row_scale[None, :, None] * sigma
    return jnp.clip(values, -1.0, 1.0).astype(jnp.bfloat16)


def block_scale(rng, shape, cuts, smallest, high):
    factor_of, own = 1.0, jax.random.fold_in(rng, 6)
    for axis_at, blocks in cuts:
        heights = jnp.exp(jax.random.uniform(jax.random.fold_in(own, axis_at), (blocks,), jnp.float32, smallest / len(cuts), high / len(cuts)))
        factor_of = factor_of * jnp.repeat(heights, shape[axis_at] // blocks).reshape([-1 if axis == axis_at else 1 for axis in range(len(shape))])
    return factor_of


def gaussian(rng, dims, width, reach, pieces=(), kind=jnp.bfloat16):
    gain = block_scale(rng, dims, pieces, -0.22, 0.18) if pieces else 1.0
    drawn = jax.random.normal(rng, dims, jnp.float32) * width * gain
    return jnp.minimum(jnp.maximum(drawn, -reach), reach).astype(kind)


def setup_inputs(seed: int = 0) -> dict:
    splits = jax.random.split(jax.random.key(seed), 4)
    return {
        "orbitals": gaussian(splits[0], (NAO, NOCC), 1.0, 6.0, ((0, 8),)),
        "projector": gaussian(splits[1], (NADM, NAO), NAO ** -0.5, 0.0390625, ((0, 4), (1, 8))),
        "integrals": draw_integrals(jax.random.fold_in(splits[3], 71), 0),
    }


def reference(orbitals, projector, integrals):
    admm = jnp.dot(projector, orbitals, preferred_element_type=jnp.float32).astype(jnp.bfloat16)

    def transform(slab):
        return jnp.dot(slab, admm, preferred_element_type=jnp.float32).astype(jnp.bfloat16)

    half = lax.map(transform, integrals)
    merged = jnp.transpose(half, (1, 0, 2)).reshape(NADM, NAUX * NOCC)
    exchange = jnp.dot(merged, merged.T, preferred_element_type=jnp.float32)
    admm_wide = admm.astype(jnp.float32)
    applied = jnp.dot(exchange, admm_wide, precision=lax.Precision.HIGHEST)
    applied_low = applied.astype(jnp.bfloat16)
    back = jnp.dot(projector.T, applied_low, preferred_element_type=jnp.float32)
    energy = -0.5 * jnp.sum(admm_wide * applied) / (NADM * NOCC)
    trace = jnp.sum(jnp.diagonal(exchange)) / NADM
    return exchange, back, energy, trace
```

```python
import functools

import jax
import jax.numpy as jnp
from jax import lax
from jax.experimental import pallas as pl
from jax.experimental.pallas import tpu as pltpu
from jax.sharding import PartitionSpec as P

MESH = pl.DeviceIdType.MESH
LIMIT = 60 * 1024 * 1024


def factor(size):
    inner = 1
    while inner * inner * 4 <= size:
        inner *= 2
    return size // inner, inner


def up(value, unit):
    return -(-value // unit) * unit


def remote(src, dst, send, recv, dev):
    return pltpu.make_async_remote_copy(
        src_ref=src, dst_ref=dst, send_sem=send, recv_sem=recv, device_id=dev, device_id_type=MESH
    )


def greet(size_x, size_y):
    gx, gy = lax.axis_index("gx"), lax.axis_index("gy")
    barrier = pltpu.get_barrier_semaphore()

    def hello(step, carry):
        other = lax.rem(gx * size_y + gy + step, size_x * size_y)
        pl.semaphore_signal(
            barrier, inc=1, device_id=(other // size_y, lax.rem(other, size_y)), device_id_type=MESH
        )
        return carry

    lax.fori_loop(1, size_x * size_y, hello, 0)
    pl.semaphore_wait(barrier, size_x * size_y - 1)


def reduce_gather_kernel(
    size_x, size_y, wide, part, out, landing, send_a, recv_a, send_z, recv_z, send_x, recv_x, send_y, recv_y, send_c, recv_c
):
    gx, gy = lax.axis_index("gx"), lax.axis_index("gy")
    num_z, num_x = factor(size_x)
    z, x = gx // num_x, lax.rem(gx, num_x)
    num_y = size_y // 2
    y, c = gy // 2, lax.rem(gy, 2)
    greet(size_x, size_y)
    outgoing = []
    for d in range(1, size_x):
        to = lax.rem(gx + d, size_x)
        copy = remote(part.at[to], landing.at[d], send_a.at[d], recv_a.at[d], (to, gy))
        copy.start()
        outgoing.append(copy)
    total = part[gx].astype(jnp.float32)
    for d in range(1, size_x):
        outgoing[d - 1].wait_recv()
        total = total + landing[d].astype(jnp.float32)
    row = gy if wide else 0
    out[row, gx] = total.astype(out.dtype)
    pending = []

    def piece(group, who):
        return out.at[group, who]

    def to_core(group, who, slot):
        if wide:
            copy = remote(piece(group, who), piece(group, who), send_c.at[slot], recv_c.at[slot], (gx, gy + 1 - 2 * c))
            copy.start()
            pending.append(copy)

    def to_y(group, who, slot):
        if wide:
            for d in range(1, num_y):
                there = lax.rem(y + d, num_y)
                copy = remote(
                    piece(group, who), piece(group, who), send_y.at[slot, d], recv_y.at[slot, d], (gx, there * 2 + c)
                )
                copy.start()
                pending.append(copy)

    for d in range(1, num_z):
        to = lax.rem(z + d, num_z) * num_x + x
        copy = remote(piece(row, gx), piece(row, gx), send_z.at[d], recv_z.at[d], (to, gy))
        copy.start()
        pending.append(copy)
    for d in range(num_z):
        src_z = lax.rem(z - d + num_z, num_z)
        who = src_z * num_x + x
        if d > 0:
            remote(piece(row, who), piece(row, who), send_z.at[d], recv_z.at[d], (gx, gy)).wait_recv()
        for e in range(1, num_x):
            to = z * num_x + lax.rem(x + e, num_x)
            copy = remote(piece(row, who), piece(row, who), send_x.at[d, e], recv_x.at[d, e], (to, gy))
            copy.start()
            pending.append(copy)
        to_y(row, who, d * num_x)
        to_core(row, who, d * num_x)
    for d in range(num_z):
        src_z = lax.rem(z - d + num_z, num_z)
        for e in range(1, num_x):
            who = src_z * num_x + lax.rem(x - e + num_x, num_x)
            remote(piece(row, who), piece(row, who), send_x.at[d, e], recv_x.at[d, e], (gx, gy)).wait_recv()
            to_y(row, who, d * num_x + e)
            to_core(row, who, d * num_x + e)
    if wide:
        for d in range(num_z):
            for e in range(num_x):
                who = lax.rem(z - d + num_z, num_z) * num_x + lax.rem(x - e + num_x, num_x)
                slot = d * num_x + e
                for f in range(1, num_y):
                    group = lax.rem(y - f + num_y, num_y) * 2 + c
                    remote(piece(group, who), piece(group, who), send_y.at[slot, f], recv_y.at[slot, f], (gx, gy)).wait_recv()
                    to_core(group, who, f * size_x + slot)
        for d in range(num_z):
            for e in range(num_x):
                who = lax.rem(z - d + num_z, num_z) * num_x + lax.rem(x - e + num_x, num_x)
                for f in range(num_y):
                    group = lax.rem(y - f + num_y, num_y) * 2 + 1 - c
                    slot = f * size_x + d * num_x + e
                    remote(piece(group, who), piece(group, who), send_c.at[slot], recv_c.at[slot], (gx, gy)).wait_recv()
    for copy in outgoing:
        copy.wait_send()
    for copy in pending:
        copy.wait_send()


def reduce_gather(part, size_x, size_y, wide, number):
    rows, cols = part.shape
    chunk = up(-(-rows // size_x), 16)
    padded = jnp.pad(part.astype(jnp.bfloat16), ((0, chunk * size_x - rows), (0, 0)))
    padded = padded.reshape(size_x, chunk, cols)
    num_z, num_x = factor(size_x)
    groups = size_y if wide else 1
    dma = pltpu.SemaphoreType.DMA
    out = pl.pallas_call(
        functools.partial(reduce_gather_kernel, size_x, size_y, wide),
        out_shape=jax.ShapeDtypeStruct((groups, size_x, chunk, cols), jnp.bfloat16),
        in_specs=[pl.BlockSpec(memory_space=pltpu.VMEM)],
        out_specs=pl.BlockSpec(memory_space=pltpu.VMEM),
        scratch_shapes=[
            pltpu.VMEM((size_x, chunk, cols), jnp.bfloat16),
            dma((size_x,)),
            dma((size_x,)),
            dma((num_z,)),
            dma((num_z,)),
            dma((num_z, num_x)),
            dma((num_z, num_x)),
            dma((size_x, size_y // 2)),
            dma((size_x, size_y // 2)),
            dma((size_x * size_y // 2,)),
            dma((size_x * size_y // 2,)),
        ],
        compiler_params=pltpu.CompilerParams(collective_id=number, has_side_effects=True, vmem_limit_bytes=LIMIT),
    )(padded)
    return out.reshape(groups, size_x * chunk, cols)[:, :rows]


def exchange_kernel(
    size_x, size_y, block, own, out, cols, rows, acc, own_sem, send_u, recv_u, send_d, recv_d, send_x, recv_x, send_y, recv_y, send_c, recv_c, row_sem
):
    gx, gy = lax.axis_index("gx"), lax.axis_index("gy")
    num_z, num_x = factor(size_x)
    z, x = gx // num_x, lax.rem(gx, num_x)
    num_y = size_y // 2
    y, c = gy // 2, lax.rem(gy, 2)
    width = out.shape[1]
    window = rows.shape[2]
    per = size_x // size_y
    root = gx // per
    root_y, root_c = root // 2, lax.rem(root, 2)
    offset = lax.rem(gx, per) * block
    first = pl.multiple_of(jnp.minimum(offset // 128 * 128, cols.shape[2] - window), 128)
    mine = gy == root
    below = (y != root_y) & (c == root_c)
    last = c != root_c
    greet(size_x, size_y)
    mypiece = pltpu.make_async_copy(own, cols.at[gx], own_sem)
    mypiece.start()
    mypiece.wait()

    def upward(k):
        who = jnp.maximum(z - k, 0) * num_x + x
        return remote(cols.at[who], cols.at[who], send_u.at[k], recv_u.at[k], (jnp.minimum(z + 1, num_z - 1) * num_x + x, gy))

    def downward(k):
        who = jnp.minimum(z + k, num_z - 1) * num_x + x
        return remote(cols.at[who], cols.at[who], send_d.at[k], recv_d.at[k], (jnp.maximum(z - 1, 0) * num_x + x, gy))

    def sideways(slot, who, e):
        to = z * num_x + lax.rem(x + e, num_x)
        return remote(cols.at[who], cols.at[who], send_x.at[slot, e], recv_x.at[slot, e], (to, gy))

    def row_y(who, f):
        return remote(
            cols.at[who, :, pl.ds(first, window)], rows.at[who], send_y.at[who, f], recv_y.at[who], (gx, lax.rem(y + f, num_y) * 2 + c)
        )

    def row_c(who, source):
        return remote(source, rows.at[who], send_c.at[who], recv_c.at[who], (gx, gy + 1 - 2 * c))

    def row_own(who):
        return pltpu.make_async_copy(cols.at[who, :, pl.ds(first, window)], rows.at[who], row_sem.at[who])

    def have(who):
        @pl.when(mine)
        def _():
            for f in range(1, num_y):
                row_y(who, f).start()
            row_c(who, cols.at[who, :, pl.ds(first, window)]).start()
            row_own(who).start()

    def spread(slot, who):
        for e in range(1, num_x):
            sideways(slot, who, e).start()
        have(who)

    for k in range(num_z):
        if k > 0:
            @pl.when(z >= k)
            def _(k=k):
                who = jnp.maximum(z - k, 0) * num_x + x
                remote(cols.at[who], cols.at[who], send_u.at[k - 1], recv_u.at[k - 1], (gx, gy)).wait_recv()
        if k < num_z - 1:
            @pl.when((z >= k) & (z < num_z - 1))
            def _(k=k):
                upward(k).start()
        if k > 0:
            @pl.when(z + k < num_z)
            def _(k=k):
                who = jnp.minimum(z + k, num_z - 1) * num_x + x
                remote(cols.at[who], cols.at[who], send_d.at[k - 1], recv_d.at[k - 1], (gx, gy)).wait_recv()
        if k < num_z - 1:
            @pl.when((z + k < num_z) & (z > 0))
            def _(k=k):
                downward(k).start()
        for side in ((1, -1) if k else (1,)):
            src_z = z - side * k
            @pl.when((src_z >= 0) & (src_z < num_z))
            def _(src_z=src_z):
                src_z = jnp.clip(src_z, 0, num_z - 1)
                spread(src_z, src_z * num_x + x)
        for side in ((1, -1) if k else (1,)):
            src_z = z - side * k
            @pl.when((src_z >= 0) & (src_z < num_z))
            def _(src_z=src_z):
                src_z = jnp.clip(src_z, 0, num_z - 1)
                for e in range(1, num_x):
                    who = src_z * num_x + lax.rem(x - e + num_x, num_x)
                    sideways(src_z, who, e).wait_recv()
                    have(who)

    def finish(who, carry):
        @pl.when(mine)
        def _():
            row_own(who).wait()

        @pl.when(below)
        def _():
            row_y(who, 1).wait_recv()
            row_c(who, rows.at[who]).start()

        @pl.when(last)
        def _():
            row_c(who, rows.at[who]).wait_recv()

        for start in range(0, width, 512):
            span = min(512, width - start)
            term = lax.dot_general(
                rows[who], cols[who, :, start:start + span], (((0,), (0,)), ((), ())), preferred_element_type=jnp.float32
            )

            @pl.when(who == 0)
            def _():
                acc[:, start:start + span] = term

            @pl.when(who > 0)
            def _():
                acc[:, start:start + span] += term
        return carry

    lax.fori_loop(0, size_x, finish, 0)
    for i in range(per):
        at = i * block - min(i * block // 128 * 128, cols.shape[2] - window)

        @pl.when(lax.rem(gx, per) == i)
        def _(at=at):
            out[...] = acc[at:at + block, :]

    for k in range(num_z - 1):
        @pl.when((z >= k) & (z < num_z - 1))
        def _(k=k):
            upward(k).wait_send()

        @pl.when((z + k < num_z) & (z > 0))
        def _(k=k):
            downward(k).wait_send()
    for src_z in range(num_z):
        for e in range(1, num_x):
            sideways(src_z, src_z * num_x + x, e).wait_send()

    def drain(who, carry):
        @pl.when(mine)
        def _():
            for f in range(1, num_y):
                row_y(who, f).wait_send()

        @pl.when(mine | below)
        def _():
            row_c(who, rows.at[who]).wait_send()

        return carry

    lax.fori_loop(0, size_x, drain, 0)


def exchange_of(half_t, size_x, size_y, block, number):
    occ, width = half_t.shape
    num_z, num_x = factor(size_x)
    per = size_x // size_y
    padded = up(width, 128)
    window = max(up(i * block % 128 + block, 128) for i in range(per))
    dma = pltpu.SemaphoreType.DMA
    half_t = jnp.pad(half_t, ((0, 0), (0, padded - width)))
    return pl.pallas_call(
        functools.partial(exchange_kernel, size_x, size_y, block),
        out_shape=jax.ShapeDtypeStruct((block, width), jnp.float32),
        in_specs=[pl.BlockSpec(memory_space=pltpu.VMEM)],
        out_specs=pl.BlockSpec(memory_space=pltpu.VMEM),
        scratch_shapes=[
            pltpu.VMEM((size_x, occ, padded), jnp.bfloat16),
            pltpu.VMEM((size_x, occ, window), jnp.bfloat16),
            pltpu.VMEM((window, width), jnp.float32),
            dma(()),
            dma((num_z,)),
            dma((num_z,)),
            dma((num_z,)),
            dma((num_z,)),
            dma((num_z, num_x)),
            dma((num_z, num_x)),
            dma((size_x, size_y // 2)),
            dma((size_x,)),
            dma((size_x,)),
            dma((size_x,)),
            dma((size_x,)),
        ],
        compiler_params=pltpu.CompilerParams(collective_id=number, has_side_effects=True, vmem_limit_bytes=LIMIT),
    )(half_t)


def on_device(size_x, size_y, orbitals, projector, integrals):
    part_rows = projector.shape[0]
    partial_value = jnp.dot(projector, orbitals, preferred_element_type=jnp.float32)
    groups = reduce_gather(partial_value, size_x, size_y, True, 1)
    occ = groups.shape[2]
    total_adm = part_rows * size_y
    admm = groups.reshape(total_adm, occ)
    half_t = lax.dot_general(
        admm, integrals[0], (((0,), (1,)), ((), ())), preferred_element_type=jnp.float32
    ).astype(jnp.bfloat16)
    exchange = exchange_of(half_t, size_x, size_y, total_adm // size_x, 2)
    own = lax.dynamic_index_in_dim(groups, lax.axis_index("gy"), 0, keepdims=False)
    mixed = lax.psum(jnp.dot(half_t, own, preferred_element_type=jnp.float32), "gy")
    wide = half_t.astype(jnp.float32)
    trace_part = jnp.sum(wide * wide)
    energy_part = jnp.sum(mixed * mixed) / size_y
    energy_total, trace_total = lax.psum((energy_part, trace_part), ("gx", "gy"))
    applied_part = lax.dot_general(
        half_t, mixed.astype(jnp.bfloat16), (((0,), (0,)), ((), ())), preferred_element_type=jnp.float32
    )
    applied_low = reduce_gather(applied_part, size_x, size_y, False, 3)[0]
    back_part = lax.dot_general(
        projector, applied_low, (((0,), (0,)), ((), ())), preferred_element_type=jnp.float32
    )
    back = lax.psum_scatter(back_part, "gy", scatter_dimension=1, tiled=True)
    energy_mean = -0.5 * energy_total / (total_adm * occ)
    trace_mean = trace_total / total_adm
    return (exchange, back, energy_mean, trace_mean)


def solution(mesh):
    return jax.shard_map(
        functools.partial(on_device, mesh.shape["gx"], mesh.shape["gy"]),
        mesh=mesh,
        in_specs=(P("gx", None), P("gy", "gx"), P("gx", "gy", None)),
        out_specs=(P("gx", "gy"), P("gx", "gy"), P(), P()),
        check_vma=False,
    )
```

```python
import functools

import jax
import jax.numpy as jnp
from jax import lax
from jax.experimental import pallas as pl
from jax.experimental.pallas import tpu as pltpu
from jax.sharding import PartitionSpec as P

MESH = pl.DeviceIdType.MESH
LIMIT = 60 * 1024 * 1024


def factor(size):
    inner = 1
    while inner * inner * 4 <= size:
        inner *= 2
    return size // inner, inner


def up(value, unit):
    return -(-value // unit) * unit


def remote(src, dst, send, recv, dev):
    return pltpu.make_async_remote_copy(
        src_ref=src, dst_ref=dst, send_sem=send, recv_sem=recv, device_id=dev, device_id_type=MESH
    )


def greet(size_x, size_y):
    gx, gy = lax.axis_index("gx"), lax.axis_index("gy")
    barrier = pltpu.get_barrier_semaphore()

    def hello(step, carry):
        other = lax.rem(gx * size_y + gy + step, size_x * size_y)
        pl.semaphore_signal(
            barrier, inc=1, device_id=(other // size_y, lax.rem(other, size_y)), device_id_type=MESH
        )
        return carry

    lax.fori_loop(1, size_x * size_y, hello, 0)
    pl.semaphore_wait(barrier, size_x * size_y - 1)


def reduce_gather_kernel(
    size_x, size_y, wide, part, out, landing, send_a, recv_a, send_z, recv_z, send_x, recv_x, send_y, recv_y, send_c, recv_c
):
    gx, gy = lax.axis_index("gx"), lax.axis_index("gy")
    num_z, num_x = factor(size_x)
    z, x = gx // num_x, lax.rem(gx, num_x)
    num_y = size_y // 2
    y, c = gy // 2, lax.rem(gy, 2)
    greet(size_x, size_y)
    outgoing = []
    for d in range(1, size_x):
        to = lax.rem(gx + d, size_x)
        copy = remote(part.at[to], landing.at[d], send_a.at[d], recv_a.at[d], (to, gy))
        copy.start()
        outgoing.append(copy)
    total = part[gx].astype(jnp.float32)
    for d in range(1, size_x):
        outgoing[d - 1].wait_recv()
        total = total + landing[d].astype(jnp.float32)
    row = gy if wide else 0
    out[row, gx] = total.astype(out.dtype)
    pending = []

    def piece(group, who):
        return out.at[group, who]

    def to_core(group, who, slot):
        if wide:
            copy = remote(piece(group, who), piece(group, who), send_c.at[slot], recv_c.at[slot], (gx, gy + 1 - 2 * c))
            copy.start()
            pending.append(copy)

    def to_y(group, who, slot):
        if wide:
            for d in range(1, num_y):
                there = lax.rem(y + d, num_y)
                copy = remote(
                    piece(group, who), piece(group, who), send_y.at[slot, d], recv_y.at[slot, d], (gx, there * 2 + c)
                )
                copy.start()
                pending.append(copy)

    for d in range(1, num_z):
        to = lax.rem(z + d, num_z) * num_x + x
        copy = remote(piece(row, gx), piece(row, gx), send_z.at[d], recv_z.at[d], (to, gy))
        copy.start()
        pending.append(copy)
    for d in range(num_z):
        src_z = lax.rem(z - d + num_z, num_z)
        who = src_z * num_x + x
        if d > 0:
            remote(piece(row, who), piece(row, who), send_z.at[d], recv_z.at[d], (gx, gy)).wait_recv()
        for e in range(1, num_x):
            to = z * num_x + lax.rem(x + e, num_x)
            copy = remote(piece(row, who), piece(row, who), send_x.at[d, e], recv_x.at[d, e], (to, gy))
            copy.start()
            pending.append(copy)
        to_y(row, who, d * num_x)
        to_core(row, who, d * num_x)
    for d in range(num_z):
        src_z = lax.rem(z - d + num_z, num_z)
        for e in range(1, num_x):
            who = src_z * num_x + lax.rem(x - e + num_x, num_x)
            remote(piece(row, who), piece(row, who), send_x.at[d, e], recv_x.at[d, e], (gx, gy)).wait_recv()
            to_y(row, who, d * num_x + e)
            to_core(row, who, d * num_x + e)
    if wide:
        for d in range(num_z):
            for e in range(num_x):
                who = lax.rem(z - d + num_z, num_z) * num_x + lax.rem(x - e + num_x, num_x)
                slot = d * num_x + e
                for f in range(1, num_y):
                    group = lax.rem(y - f + num_y, num_y) * 2 + c
                    remote(piece(group, who), piece(group, who), send_y.at[slot, f], recv_y.at[slot, f], (gx, gy)).wait_recv()
                    to_core(group, who, f * size_x + slot)
        for d in range(num_z):
            for e in range(num_x):
                who = lax.rem(z - d + num_z, num_z) * num_x + lax.rem(x - e + num_x, num_x)
                for f in range(num_y):
                    group = lax.rem(y - f + num_y, num_y) * 2 + 1 - c
                    slot = f * size_x + d * num_x + e
                    remote(piece(group, who), piece(group, who), send_c.at[slot], recv_c.at[slot], (gx, gy)).wait_recv()
    for copy in outgoing:
        copy.wait_send()
    for copy in pending:
        copy.wait_send()


def reduce_gather(part, size_x, size_y, wide, number):
    rows, cols = part.shape
    chunk = up(-(-rows // size_x), 16)
    padded = jnp.pad(part.astype(jnp.bfloat16), ((0, chunk * size_x - rows), (0, 0)))
    padded = padded.reshape(size_x, chunk, cols)
    num_z, num_x = factor(size_x)
    groups = size_y if wide else 1
    dma = pltpu.SemaphoreType.DMA
    out = pl.pallas_call(
        functools.partial(reduce_gather_kernel, size_x, size_y, wide),
        out_shape=jax.ShapeDtypeStruct((groups, size_x, chunk, cols), jnp.bfloat16),
        in_specs=[pl.BlockSpec(memory_space=pltpu.VMEM)],
        out_specs=pl.BlockSpec(memory_space=pltpu.VMEM),
        scratch_shapes=[
            pltpu.VMEM((size_x, chunk, cols), jnp.bfloat16),
            dma((size_x,)),
            dma((size_x,)),
            dma((num_z,)),
            dma((num_z,)),
            dma((num_z, num_x)),
            dma((num_z, num_x)),
            dma((size_x, size_y // 2)),
            dma((size_x, size_y // 2)),
            dma((size_x * size_y // 2,)),
            dma((size_x * size_y // 2,)),
        ],
        compiler_params=pltpu.CompilerParams(collective_id=number, has_side_effects=True, vmem_limit_bytes=LIMIT),
    )(padded)
    return out.reshape(groups, size_x * chunk, cols)[:, :rows]


def exchange_kernel(
    size_x, size_y, block, own, stats, out, sums, cols, rows, acc, landing, send_s, recv_s, own_sem, send_u, recv_u, send_d, recv_d, send_x, recv_x, send_y, recv_y, send_c, recv_c, row_sem
):
    gx, gy = lax.axis_index("gx"), lax.axis_index("gy")
    num_z, num_x = factor(size_x)
    z, x = gx // num_x, lax.rem(gx, num_x)
    num_y = size_y // 2
    y, c = gy // 2, lax.rem(gy, 2)
    width = out.shape[1]
    window = rows.shape[2]
    per = size_x // size_y
    root = gx // per
    root_y, root_c = root // 2, lax.rem(root, 2)
    offset = lax.rem(gx, per) * block
    first = pl.multiple_of(jnp.minimum(offset // 128 * 128, cols.shape[2] - window), 128)
    mine = gy == root
    below = (y != root_y) & (c == root_c)
    last = c != root_c
    greet(size_x, size_y)
    mypiece = pltpu.make_async_copy(own, cols.at[gx], own_sem)
    mypiece.start()
    mypiece.wait()
    devices = size_x * size_y
    me = gx * size_y + gy

    def stat_copy(slot, step, to):
        return remote(stats, landing.at[slot], send_s.at[step], recv_s.at[slot], (to // size_y, lax.rem(to, size_y)))

    def upward(k):
        who = jnp.maximum(z - k, 0) * num_x + x
        return remote(cols.at[who], cols.at[who], send_u.at[k], recv_u.at[k], (jnp.minimum(z + 1, num_z - 1) * num_x + x, gy))

    def downward(k):
        who = jnp.minimum(z + k, num_z - 1) * num_x + x
        return remote(cols.at[who], cols.at[who], send_d.at[k], recv_d.at[k], (jnp.maximum(z - 1, 0) * num_x + x, gy))

    def sideways(slot, who, e):
        to = z * num_x + lax.rem(x + e, num_x)
        return remote(cols.at[who], cols.at[who], send_x.at[slot, e], recv_x.at[slot, e], (to, gy))

    def row_y(who, f):
        return remote(
            cols.at[who, :, pl.ds(first, window)], rows.at[who], send_y.at[who, f], recv_y.at[who], (gx, lax.rem(y + f, num_y) * 2 + c)
        )

    def row_c(who, source):
        return remote(source, rows.at[who], send_c.at[who], recv_c.at[who], (gx, gy + 1 - 2 * c))

    def row_own(who):
        return pltpu.make_async_copy(cols.at[who, :, pl.ds(first, window)], rows.at[who], row_sem.at[who])

    def have(who):
        @pl.when(mine)
        def _():
            for f in range(1, num_y):
                row_y(who, f).start()
            row_c(who, cols.at[who, :, pl.ds(first, window)]).start()
            row_own(who).start()

    def spread(slot, who):
        for e in range(1, num_x):
            sideways(slot, who, e).start()
        have(who)

    def add_term(who, fresh):
        @pl.when(mine)
        def _():
            row_own(who).wait()

        @pl.when(below)
        def _():
            row_y(who, 1).wait_recv()
            row_c(who, rows.at[who]).start()

        @pl.when(last)
        def _():
            row_c(who, rows.at[who]).wait_recv()

        for start in range(0, width, 512):
            span = min(512, width - start)
            term = lax.dot_general(
                rows[who], cols[who, :, start:start + span], (((0,), (0,)), ((), ())), preferred_element_type=jnp.float32
            )
            if fresh:
                acc[:, start:start + span] = term
            else:
                acc[:, start:start + span] += term

    def add_terms(k):
        if k == 0:
            add_term(gx, True)

        def one(i, carry):
            src_z = z + jnp.where(i < num_x, -k, k)

            @pl.when((src_z >= 0) & (src_z < num_z))
            def _():
                add_term(src_z * num_x + lax.rem(x + lax.rem(i, num_x), num_x), False)

            return carry

        lax.fori_loop(0 if k else 1, 2 * num_x if k else num_x, one, 0)

    for k in range(num_z):
        if k > 0:
            @pl.when(z >= k)
            def _(k=k):
                who = jnp.maximum(z - k, 0) * num_x + x
                remote(cols.at[who], cols.at[who], send_u.at[k - 1], recv_u.at[k - 1], (gx, gy)).wait_recv()
        if k < num_z - 1:
            @pl.when((z >= k) & (z < num_z - 1))
            def _(k=k):
                upward(k).start()
        if k > 0:
            @pl.when(z + k < num_z)
            def _(k=k):
                who = jnp.minimum(z + k, num_z - 1) * num_x + x
                remote(cols.at[who], cols.at[who], send_d.at[k - 1], recv_d.at[k - 1], (gx, gy)).wait_recv()
        if k < num_z - 1:
            @pl.when((z + k < num_z) & (z > 0))
            def _(k=k):
                downward(k).start()
        for side in ((1, -1) if k else (1,)):
            src_z = z - side * k
            @pl.when((src_z >= 0) & (src_z < num_z))
            def _(src_z=src_z):
                src_z = jnp.clip(src_z, 0, num_z - 1)
                spread(src_z, src_z * num_x + x)
        if k == 0:
            def tell(step, carry):
                stat_copy(me, step, lax.rem(me + step, devices)).start()
                return carry

            lax.fori_loop(1, devices, tell, 0)
        else:
            add_terms(k - 1)
        for side in ((1, -1) if k else (1,)):
            src_z = z - side * k
            @pl.when((src_z >= 0) & (src_z < num_z))
            def _(src_z=src_z):
                src_z = jnp.clip(src_z, 0, num_z - 1)
                for e in range(1, num_x):
                    who = src_z * num_x + lax.rem(x - e + num_x, num_x)
                    sideways(src_z, who, e).wait_recv()
                    have(who)
    add_terms(num_z - 1)

    def hear(step, carry):
        stat_copy(lax.rem(me + step, devices), step, me).wait_recv()
        return carry

    lax.fori_loop(1, devices, hear, 0)
    landing[me] = stats[...]
    sums[...] = jnp.sum(landing[...], axis=0)

    def told(step, carry):
        stat_copy(me, step, me).wait_send()
        return carry

    lax.fori_loop(1, devices, told, 0)
    for i in range(per):
        at = i * block - min(i * block // 128 * 128, cols.shape[2] - window)

        @pl.when(lax.rem(gx, per) == i)
        def _(at=at):
            out[...] = acc[at:at + block, :]

    for k in range(num_z - 1):
        @pl.when((z >= k) & (z < num_z - 1))
        def _(k=k):
            upward(k).wait_send()

        @pl.when((z + k < num_z) & (z > 0))
        def _(k=k):
            downward(k).wait_send()
    for src_z in range(num_z):
        for e in range(1, num_x):
            sideways(src_z, src_z * num_x + x, e).wait_send()

    def drain(who, carry):
        @pl.when(mine)
        def _():
            for f in range(1, num_y):
                row_y(who, f).wait_send()

        @pl.when(mine | below)
        def _():
            row_c(who, rows.at[who]).wait_send()

        return carry

    lax.fori_loop(0, size_x, drain, 0)


def exchange_of(half_t, stats, size_x, size_y, block, number):
    occ, width = half_t.shape
    num_z, num_x = factor(size_x)
    per = size_x // size_y
    padded = up(width, 128)
    window = max(up(i * block % 128 + block, 128) for i in range(per))
    dma = pltpu.SemaphoreType.DMA
    half_t = jnp.pad(half_t, ((0, 0), (0, padded - width)))
    return pl.pallas_call(
        functools.partial(exchange_kernel, size_x, size_y, block),
        out_shape=(jax.ShapeDtypeStruct((block, width), jnp.float32), jax.ShapeDtypeStruct(stats.shape, jnp.float32)),
        in_specs=[pl.BlockSpec(memory_space=pltpu.VMEM)] * 2,
        out_specs=[pl.BlockSpec(memory_space=pltpu.VMEM)] * 2,
        scratch_shapes=[
            pltpu.VMEM((size_x, occ, padded), jnp.bfloat16),
            pltpu.VMEM((size_x, occ, window), jnp.bfloat16),
            pltpu.VMEM((window, width), jnp.float32),
            pltpu.VMEM((size_x * size_y,) + stats.shape, jnp.float32),
            dma((size_x * size_y,)),
            dma((size_x * size_y,)),
            dma(()),
            dma((num_z,)),
            dma((num_z,)),
            dma((num_z,)),
            dma((num_z,)),
            dma((num_z, num_x)),
            dma((num_z, num_x)),
            dma((size_x, size_y // 2)),
            dma((size_x,)),
            dma((size_x,)),
            dma((size_x,)),
            dma((size_x,)),
        ],
        compiler_params=pltpu.CompilerParams(collective_id=number, has_side_effects=True, vmem_limit_bytes=LIMIT),
    )(half_t, stats)


def sum_kernel(size_y, same, part, out, landing, send, recv):
    gx, gy = lax.axis_index("gx"), lax.axis_index("gy")
    barrier = pltpu.get_barrier_semaphore()
    for d in range(1, size_y):
        pl.semaphore_signal(barrier, inc=1, device_id=(gx, lax.rem(gy + d, size_y)), device_id_type=MESH)
    pl.semaphore_wait(barrier, size_y - 1)
    copies = []
    for d in range(1, size_y):
        to = lax.rem(gy + d, size_y)
        copy = remote(part.at[0 if same else to], landing.at[d], send.at[d], recv.at[d], (gx, to))
        copy.start()
        copies.append(copy)
    total = part[0 if same else gy].astype(jnp.float32)
    for d in range(1, size_y):
        copies[d - 1].wait_recv()
        total = total + landing[d].astype(jnp.float32)
    out[...] = total
    for copy in copies:
        copy.wait_send()


def sum_over_y(part, size_y, same, number):
    shape = part.shape[1:]
    dma = pltpu.SemaphoreType.DMA
    return pl.pallas_call(
        functools.partial(sum_kernel, size_y, same),
        out_shape=jax.ShapeDtypeStruct(shape, jnp.float32),
        in_specs=[pl.BlockSpec(memory_space=pltpu.VMEM)],
        out_specs=pl.BlockSpec(memory_space=pltpu.VMEM),
        scratch_shapes=[pltpu.VMEM((size_y,) + shape, part.dtype), dma((size_y,)), dma((size_y,))],
        compiler_params=pltpu.CompilerParams(collective_id=number, has_side_effects=True, vmem_limit_bytes=LIMIT),
    )(part)


def on_device(size_x, size_y, orbitals, projector, integrals):
    part_rows = projector.shape[0]
    partial_value = jnp.dot(projector, orbitals, preferred_element_type=jnp.float32)
    groups = reduce_gather(partial_value, size_x, size_y, True, 1)
    occ = groups.shape[2]
    total_adm = part_rows * size_y
    admm = groups.reshape(total_adm, occ)
    half_t = lax.dot_general(
        admm, integrals[0], (((0,), (1,)), ((), ())), preferred_element_type=jnp.float32
    ).astype(jnp.bfloat16)
    own = lax.dynamic_index_in_dim(groups, lax.axis_index("gy"), 0, keepdims=False)
    mixed_part = jnp.dot(half_t, own, preferred_element_type=jnp.float32)
    mixed = sum_over_y(mixed_part[None], size_y, True, 4)
    wide = half_t.astype(jnp.float32)
    trace_part = jnp.sum(wide * wide)
    energy_part = jnp.sum(mixed * mixed) / size_y
    lane = lax.broadcasted_iota(jnp.int32, (8, 128), 1)
    stats = jnp.where(lane == 0, energy_part, jnp.where(lane == 1, trace_part, 0.0))
    applied_part = lax.dot_general(
        half_t, mixed.astype(jnp.bfloat16), (((0,), (0,)), ((), ())), preferred_element_type=jnp.float32
    )
    applied_low = reduce_gather(applied_part, size_x, size_y, False, 3)[0]
    back_part = lax.dot_general(
        applied_low, projector, (((0,), (0,)), ((), ())), preferred_element_type=jnp.float32
    ).astype(jnp.bfloat16)
    back = sum_over_y(back_part.reshape(size_y, occ // size_y, -1), size_y, False, 5).T
    exchange, sums = exchange_of(half_t, stats, size_x, size_y, total_adm // size_x, 2)
    energy_total, trace_total = sums[0, 0], sums[0, 1]
    energy_mean = -0.5 * energy_total / (total_adm * occ)
    trace_mean = trace_total / total_adm
    return (exchange, back, energy_mean, trace_mean)


def solution(mesh):
    return jax.shard_map(
        functools.partial(on_device, mesh.shape["gx"], mesh.shape["gy"]),
        mesh=mesh,
        in_specs=(P("gx", None), P("gy", "gx"), P("gx", "gy", None)),
        out_specs=(P("gx", "gy"), P("gx", "gy"), P(), P()),
        check_vma=False,
    )
```
